32 devices in a mesh: row: 4 (over x, core), col: 4 (over z), depth: 2 (over y).
Axes of the slice: x: 2, y: 2, z: 4, core: 2. Of those that a mesh axis runs over, the one named last changes fastest.
Arguments:
- trailing: float32 [3008, 48128], P('depth', ('row', 'col')), may hold values from -6 to 6
- panel_block: float32 [48128, 1024], P(('row', 'col', 'depth')), may hold values from -6 to 6
- factor_panel: float32 [48128, 1024], P(('row', 'col', 'depth')), may hold values from -0.1875 to 0.1875
- corner_block: float32 [1024, 1024], P(('row', 'col', 'depth')), may hold values from -6 to 6, as said below
- corner_inverse: float32 [1024, 1024], P(('row', 'col', 'depth')), may hold values from -1 to 2, as said below
Outputs:
- trailing_out: float32 [3008, 48128], P('depth', ('row', 'col'))
- panel_out: float32 [48128, 1024], P(('row', 'col', 'depth'))
- corner_out: float32 [1024, 1024], P(('row', 'col', 'depth'))
The draws below stay inside these ranges and needn't reach their ends.
Inputs may be any that keep to these rules, and one draw needn't show every extreme that they name: `corner_block`: symmetric. `corner_inverse`: lower triangular, diagonal between 1 and 2.
All inputs are finite; a program needn't handle non-finite values.
Results may differ from the reference program's by a relative error of at most 0.00012.
Values sent between devices are 32-bit elements; how exact they have to be, the bound alone decides.
No kernel may reach another device: no remote copies, remote signals or barrier semaphores. Data moves between devices by JAX's collectives and lax.ppermute only.
A program may use at most 192 MiB of HBM per device.

```python
import jax
import jax.numpy as jnp
from jax import lax

NB = 1024
M = 48128
SPAN = 1
SLAB = 3008
N_DEPTH = 2


def draw_corner_block(key, part):
    noise = jax.random.truncated_normal(jax.random.fold_in(key, 11), -4.0, 4.0, (NB, NB), jnp.float32)
    return (noise + noise.T) * 0.7071


def draw_corner_inverse(key, part):
    below = jax.random.truncated_normal(jax.random.fold_in(key, 23), -4.0, 4.0, (NB, NB), jnp.float32)
    diagonal = jax.random.uniform(jax.random.fold_in(key, 29), (NB,), jnp.float32, 1.0, 2.0)
    strict = jnp.tril(below, -1) * (0.5 / NB ** 0.5)
    return strict + jnp.diag(diagonal)


def block_scale(rng, shape, cuts, least, largest):
    level = 1.0
    for position, shards_of in cuts:
        draws = jax.random.uniform(jax.random.fold_in(jax.random.fold_in(rng, 6), position), (shards_of,), jnp.float32, least / len(cuts), largest / len(cuts))
        level = level * jnp.repeat(jnp.exp(draws), shape[position] // shards_of).reshape((-1,) + (1,) * (len(shape) - 1 - position))
    return level


def gaussian(stream_key, shape, scale, limit, cuts=(), dtype=jnp.bfloat16):
    loudness = block_scale(stream_key, shape, cuts, -0.22, 0.18) if cuts else 1.0
    array = jax.random.normal(stream_key, shape, jnp.float32) * scale * loudness
    return jnp.minimum(jnp.maximum(array, -limit), limit).astype(dtype)


def setup_inputs(seed: int = 0) -> dict:
    arg_keys = jax.random.split(jax.random.key(seed), 6)
    trailing = gaussian(arg_keys[0], (SLAB, M), 1.0, 6.0, ((0, 2), (1, 16)), jnp.float32)
    panel_block = gaussian(arg_keys[1], (M, NB), 1.0, 6.0, ((0, 32),), jnp.float32)
    factor_panel = gaussian(arg_keys[2], (M, NB), NB ** -0.5, 0.1875, ((0, 32),), jnp.float32)
    corner_block = draw_corner_block(jax.random.fold_in(arg_keys[5], 71), 0)
    corner_inverse = draw_corner_inverse(jax.random.fold_in(arg_keys[5], 71), 0)
    return dict(trailing=trailing, panel_block=panel_block, factor_panel=factor_panel, corner_block=corner_block, corner_inverse=corner_inverse)


def matmul(left, right):
    return jnp.dot(left, right, precision=lax.Precision.HIGHEST, preferred_element_type=jnp.float32)


def permute(matrix):
    block = matrix[:SLAB]
    shaped = block.reshape(SPAN, N_DEPTH, SLAB // (SPAN * N_DEPTH), block.shape[1])
    return jnp.transpose(shaped, (1, 0, 2, 3)).reshape(SLAB, block.shape[1])


def reference(trailing, panel_block, factor_panel, corner_block, corner_inverse):
    corner_out = matmul(corner_inverse, matmul(corner_block, corner_inverse.T))
    scaled = matmul(panel_block, corner_inverse.T)
    coupling = matmul(factor_panel, corner_out)
    half_panel = scaled - 0.5 * coupling
    panel_out = half_panel - 0.5 * coupling
    update = matmul(permute(half_panel), factor_panel.T) + matmul(permute(factor_panel), half_panel.T)
    trailing_out = trailing - update
    return trailing_out, panel_out, corner_out
```

```python
import functools

import jax
import jax.numpy as jnp
from jax import lax
from jax.experimental import pallas as pl
from jax.experimental.pallas import tpu as pltpu
from jax.sharding import PartitionSpec as P


ALL = ("row", "col", "depth")
PLANE = ("row", "col")
TILE = 256
BAND = 768
SWAP = [(0, 1), (1, 0)]
LANES = (((1,), (1,)), ((), ()))


def matmul(left, right, precision=lax.Precision.HIGH):
    return jnp.dot(left, right, precision=precision, preferred_element_type=jnp.float32)


def contract(left, right, precision=lax.Precision.HIGH):
    return lax.dot_general(
        left, right, LANES, precision=precision, preferred_element_type=jnp.float32
    )


def split(value):
    high = value.astype(jnp.bfloat16)
    return high, (value - high.astype(jnp.float32)).astype(jnp.bfloat16)


def transform(panel_rows, factor_rows, block, inverse):
    turned = matmul(factor_rows, inverse)
    return turned, contract(panel_rows - matmul(turned, block), inverse)


def corner_gather(corner_block, corner_inverse, n_depth):
    share, size = corner_block.shape
    first = lax.axis_index(ALL) * share
    row = first + lax.broadcasted_iota(jnp.int32, (share, size), 0)
    col = lax.broadcasted_iota(jnp.int32, (share, size), 1)
    square = jnp.where(col > row, corner_block, corner_inverse)
    diagonal = jnp.sum(jnp.where(col == row, corner_block, 0.0), axis=0, keepdims=True)
    mine = jnp.concatenate([square, diagonal])
    if n_depth == 2:
        other = lax.ppermute(mine, "depth", SWAP)
        lower = lax.axis_index("depth") == 0
        pair = jnp.stack([jnp.where(lower, mine, other), jnp.where(lower, other, mine)])
    else:
        pair = lax.all_gather(mine, "depth", axis=0)
    full = lax.all_gather(pair, PLANE, axis=0)
    square = full[:, :, :share].reshape(size, size)
    diagonal = jnp.sum(full[:, :, share], axis=(0, 1))
    row = lax.broadcasted_iota(jnp.int32, (size, size), 0)
    col = lax.broadcasted_iota(jnp.int32, (size, size), 1)
    block = jnp.where(col > row, square, jnp.where(col < row, square.T, diagonal[None]))
    return block, jnp.where(col > row, 0.0, square)


def slab_piece(panel_block, factor_panel, slab, n_row, n_col):
    row, col = lax.axis_index("row"), lax.axis_index("col")
    half = n_row // 2 if n_row % 2 == 0 else n_row
    groups = n_row // half
    share = -(-slab // (n_row * n_col * 8)) * 8

    def device(r, c):
        return r * n_col + c

    def take(value, r, c):
        start = min(device(r, c) * share, slab)
        stop = min(start + share, slab)
        return jnp.pad(value[start:stop], ((0, share - stop + start), (0, 0)))

    def pieces(group, place):
        return jnp.stack(
            [
                jnp.stack([take(v, group * half + k, place) for v in (panel_block, factor_panel)])
                for k in range(half)
            ]
        )

    across = {}
    for c in reversed(range(n_col)):
        across[c] = pieces(0, c)
        if groups > 1:
            sent = lax.ppermute(pieces(1, c), PLANE, [(0, device(half, 0))])
            across[c] = jnp.where(row == 0, across[c], sent)
    held = jnp.where(col == 0, across[0], 0.0)
    for c in reversed(range(1, n_col)):
        pairs = [(device(g * half, 0), device(g * half, c)) for g in range(groups)]
        held = held + lax.ppermute(across[c], PLANE, pairs)
    mine = jnp.where(row % half == 0, held[0], 0.0)
    for k in range(1, half):
        pairs = [
            (device(g * half, c), device(g * half + k, c))
            for g in range(groups)
            for c in range(n_col)
        ]
        mine = mine + lax.ppermute(held[k], PLANE, pairs)
    return mine


def update_kernel(place, slab_ref, factor_ref, panel_ref, trailing_ref, *rest):
    out_ref, left, right = rest[-3:]
    width = factor_ref.shape[1]

    @pl.when(pl.program_id(0) == 0)
    def _():
        for part in range(2):
            top, low = split(slab_ref[:, part].reshape(-1, width))
            for slot, value in enumerate((top, top, low)):
                left[:, pl.ds((2 * slot + part) * width, width)] = value

    for part, ref in enumerate((factor_ref, panel_ref)):
        top, low = split(ref[...])
        for slot, value in enumerate((top, low, top)):
            right[:, pl.ds((2 * slot + part) * width, width)] = value

    def band(index, carry):
        lines = pl.ds(pl.multiple_of(index * BAND, BAND), BAND)
        total = lax.dot_general(
            left[lines], right[...], LANES, preferred_element_type=jnp.float32
        )
        out_ref[lines] = trailing_ref[lines] - total
        return carry

    lax.fori_loop(0, left.shape[0] // BAND, band, 0)


def update(place, slab, factor_rows, panel_rows, trailing, previous):
    share = slab.shape[0] * slab.shape[2]
    width = slab.shape[3]
    rows = trailing.shape[0]
    tiles = place.shape[0]
    column_tile = pl.BlockSpec((share, TILE), lambda step, place: (0, place[step]))
    row_tile = pl.BlockSpec((TILE, width), lambda step, place: (step, 0))
    whole = pl.BlockSpec(
        slab.shape, lambda step, place: (0, 0, 0, 0), pipeline_mode=pl.Buffered(1)
    )
    operands = (place, slab, factor_rows, panel_rows, trailing)
    in_specs = [whole, row_tile, row_tile, column_tile]
    aliases = {}
    if previous is not None:
        operands += (previous,)
        in_specs.append(pl.BlockSpec(memory_space=pl.ANY))
        aliases = {5: 0}
    return pl.pallas_call(
        update_kernel,
        out_shape=jax.ShapeDtypeStruct(trailing.shape, trailing.dtype),
        grid_spec=pltpu.PrefetchScalarGridSpec(
            num_scalar_prefetch=1,
            grid=(tiles,),
            in_specs=in_specs,
            out_specs=column_tile,
            scratch_shapes=[
                pltpu.VMEM((share, 6 * width), jnp.bfloat16),
                pltpu.VMEM((TILE, 6 * width), jnp.bfloat16),
            ],
        ),
        input_output_aliases=aliases,
        compiler_params=pltpu.CompilerParams(vmem_limit_bytes=60 * 2**20),
        cost_estimate=pl.CostEstimate(
            flops=6 * tiles * TILE * rows * 2 * width,
            bytes_accessed=4 * (tiles * TILE * (2 * rows + 2 * width) + 2 * rows * width),
            transcendentals=0,
        ),
    )(*operands)


def corner_rows(corner_inverse, block, inverse):
    exact = lax.Precision.HIGHEST
    return contract(matmul(corner_inverse, block, exact), inverse, exact)


def plain(trailing, panel_block, factor_panel, corner_block, corner_inverse):
    slab = trailing.shape[0]
    sources = [lax.axis_index(a) == 0 for a in PLANE]

    def broadcast(value):
        return lax.psum(jnp.where(sources[0] & sources[1], value, 0.0), PLANE)

    block, inverse = corner_gather(corner_block, corner_inverse, 0)
    corner_out = corner_rows(corner_inverse, block, inverse)
    turned, panel_out = transform(panel_block, factor_panel, block, inverse)
    panel_cols = lax.all_gather(panel_block, "depth", axis=0, tiled=True)
    factor_cols = lax.all_gather(factor_panel, "depth", axis=0, tiled=True)
    panel_piece, turned_piece = broadcast(panel_out[:slab]), broadcast(turned[:slab])
    change = contract(panel_piece, factor_cols) + contract(turned_piece, panel_cols)
    return trailing - change, panel_out, corner_out


def paired(n_row, n_col, trailing, panel_block, factor_panel, corner_block, corner_inverse):
    slab = trailing.shape[0]
    count = panel_block.shape[0]
    lower = lax.axis_index("depth") == 0

    tiles = -(-2 * count // TILE)
    lead = -count % TILE
    full = (count - lead) // TILE - 1
    cut = lead + full * TILE
    factor_other = lax.ppermute(factor_panel, "depth", SWAP)
    panel_early = lax.ppermute(panel_block[:cut], "depth", SWAP)
    panel_late = lax.ppermute(panel_block[cut:], "depth", SWAP)

    block, inverse = corner_gather(corner_block, corner_inverse, 2)
    piece = slab_piece(panel_block, factor_panel, slab, n_row, n_col)
    piece_turned, piece_panel = transform(piece[0], piece[1], block, inverse)
    slab_rows = lax.all_gather(jnp.stack([piece_panel, piece_turned]), PLANE, axis=0)

    _, panel_out = transform(panel_block, factor_panel, block, inverse)
    corner_out = corner_rows(corner_inverse, block, inverse)

    def padded(rows, size):
        value = jnp.concatenate(rows)
        return jnp.pad(value, ((0, size - value.shape[0]), (0, 0)))

    upper = -(-count // TILE)
    first_low = (count + cut) // TILE
    first_tiles = full + tiles - upper
    assert first_low == first_tiles
    last_tiles = tiles - first_tiles

    def first_rows(own, part):
        size = first_tiles * TILE
        low = padded([own, part], size)
        high = padded([part[: full * TILE], own[lead:]], size)
        return jnp.where(lower, low, high)

    def last_rows(own, part, rest):
        size = last_tiles * TILE
        low = padded([rest], size)
        high = padded([part[full * TILE :], rest, own[:lead]], size)
        return jnp.where(lower, low, high)

    low_order = jnp.arange(tiles)
    high_order = jnp.concatenate(
        [jnp.arange(full), jnp.arange(upper, tiles), jnp.arange(full, upper)]
    )
    order = jnp.where(lower, low_order, high_order).astype(jnp.int32)
    out = update(
        order[:first_tiles],
        slab_rows,
        first_rows(factor_panel, factor_other[:cut]),
        first_rows(panel_block, panel_early),
        trailing,
        None,
    )
    out = update(
        order[first_tiles:],
        slab_rows,
        last_rows(factor_panel, factor_other[:cut], factor_other[cut:]),
        last_rows(panel_block, panel_early, panel_late),
        trailing,
        out,
    )
    return out, panel_out, corner_out


def paired_fits(n_row, n_depth, trailing, panel_block):
    count = panel_block.shape[0]
    fits = trailing.shape[1] == 2 * count and trailing.shape[0] <= count
    return n_depth == 2 and n_row % 2 == 0 and fits and count % 32 == 0 and count >= 4 * TILE


def body(n_row, n_col, n_depth, trailing, panel_block, *rest):
    if paired_fits(n_row, n_depth, trailing, panel_block):
        return paired(n_row, n_col, trailing, panel_block, *rest)
    return plain(trailing, panel_block, *rest)


def solution(mesh):
    in_specs = (P("depth", PLANE),) + (P(ALL, None),) * 4
    out_specs = (P("depth", PLANE), P(ALL, None), P(ALL, None))
    sizes = [mesh.shape[a] for a in ALL]
    return jax.shard_map(
        functools.partial(body, *sizes),
        mesh=mesh,
        in_specs=in_specs,
        out_specs=out_specs,
        check_vma=False,
    )
```

```python
import functools
import math

import jax
import jax.numpy as jnp
from jax import lax
from jax.experimental import pallas as pl
from jax.experimental.pallas import tpu as pltpu
from jax.sharding import PartitionSpec as P


ALL = ("row", "col", "depth")
PLANE = ("row", "col")
TILE = 256
BAND = 768
SWAP = [(0, 1), (1, 0)]
LANES = (((1,), (1,)), ((), ()))


def matmul(left, right, precision=lax.Precision.HIGH):
    return jnp.dot(left, right, precision=precision, preferred_element_type=jnp.float32)


def contract(left, right, precision=lax.Precision.HIGH):
    return lax.dot_general(
        left, right, LANES, precision=precision, preferred_element_type=jnp.float32
    )


def split(value):
    high = value.astype(jnp.bfloat16)
    return high, (value - high.astype(jnp.float32)).astype(jnp.bfloat16)


def transform(panel_rows, factor_rows, block, inverse):
    turned = matmul(factor_rows, inverse)
    return turned, contract(panel_rows - matmul(turned, block), inverse)


def transform_with_corner(panel_rows, factor_rows, corner_inverse, block, inverse):
    count = panel_rows.shape[0]
    turned = matmul(factor_rows, inverse)
    middle = matmul(jnp.concatenate([turned, corner_inverse]), block)
    rest = jnp.concatenate([panel_rows - middle[:count], middle[count:]])
    result = contract(rest, inverse)
    return turned, result[:count], result[count:]


def corner_gather(corner_block, corner_inverse, n_depth):
    share, size = corner_block.shape
    first = lax.axis_index(ALL) * share
    row = first + lax.broadcasted_iota(jnp.int32, (share, size), 0)
    col = lax.broadcasted_iota(jnp.int32, (share, size), 1)
    square = jnp.where(col > row, corner_block, corner_inverse)
    diagonal = jnp.sum(jnp.where(col == row, corner_block, 0.0), axis=0, keepdims=True)
    mine = jnp.concatenate([square, diagonal])
    if n_depth == 2:
        other = lax.ppermute(mine, "depth", SWAP)
        lower = lax.axis_index("depth") == 0
        pair = jnp.stack([jnp.where(lower, mine, other), jnp.where(lower, other, mine)])
    else:
        pair = lax.all_gather(mine, "depth", axis=0)
    full = lax.all_gather(pair, PLANE, axis=0)
    square = full[:, :, :share].reshape(size, size)
    diagonal = jnp.sum(full[:, :, share], axis=(0, 1))
    row = lax.broadcasted_iota(jnp.int32, (size, size), 0)
    col = lax.broadcasted_iota(jnp.int32, (size, size), 1)
    block = jnp.where(col > row, square, jnp.where(col < row, square.T, diagonal[None]))
    return block, jnp.where(col > row, 0.0, square)


def slab_piece(panel_block, factor_panel, slab, n_row, n_col):
    row, col = lax.axis_index("row"), lax.axis_index("col")
    half = n_row // 2
    groups = 2
    share = -(-slab // (n_row * n_col * 8)) * 8

    def device(r, c):
        return r * n_col + c

    def pieces(group, place):
        start = min((group * n_col + place) * half * share, slab)
        stop = min(start + half * share, slab)
        rows = ((0, half * share - stop + start), (0, 0))
        return jnp.stack([jnp.pad(v[start:stop], rows) for v in (panel_block, factor_panel)])

    across = {}
    for c in reversed(range(n_col)):
        sent = lax.ppermute(pieces(1, c), PLANE, [(0, device(half, 0))])
        across[c] = jnp.where(row == 0, pieces(0, c), sent)
    held = jnp.where(col == 0, across[0], 0.0)
    for c in reversed(range(1, n_col)):
        pairs = [(device(g * half, 0), device(g * half, c)) for g in range(groups)]
        held = held + lax.ppermute(across[c], PLANE, pairs)
    mine = jnp.where(row % half == 0, held[:, :share], 0.0)
    for k in range(1, half):
        pairs = [
            (device(g * half, c), device(g * half + k, c))
            for g in range(groups)
            for c in range(n_col)
        ]
        mine = mine + lax.ppermute(held[:, k * share : (k + 1) * share], PLANE, pairs)
    return mine


def lay_slab(slab_ref, left):
    groups, half, columns, parts, share, width = slab_ref.shape
    for g in range(groups):
        for k in range(half):
            for c in range(columns):
                lines = pl.ds(((g * columns + c) * half + k) * share, share)
                for part in range(parts):
                    top, low = split(slab_ref[g, k, c, part])
                    for slot, value in enumerate((top, top, low)):
                        left[lines, pl.ds((2 * slot + part) * width, width)] = value


def update_kernel(place, slab_ref, factor_ref, panel_ref, trailing_ref, *rest):
    out_ref, left, right = rest[-3:]
    width = factor_ref.shape[1]

    @pl.when(pl.program_id(0) == 0)
    def _():
        lay_slab(slab_ref, left)

    for part, ref in enumerate((factor_ref, panel_ref)):
        top, low = split(ref[...])
        for slot, value in enumerate((top, low, top)):
            right[:, pl.ds((2 * slot + part) * width, width)] = value

    def band(index, carry):
        lines = pl.ds(pl.multiple_of(index * BAND, BAND), BAND)
        total = lax.dot_general(
            left[lines], right[...], LANES, preferred_element_type=jnp.float32
        )
        out_ref[lines] = trailing_ref[lines] - total
        return carry

    lax.fori_loop(0, left.shape[0] // BAND, band, 0)


def update(place, slab, factor_rows, panel_rows, trailing, previous):
    share = math.prod(slab.shape[:3]) * slab.shape[4]
    width = slab.shape[5]
    rows = trailing.shape[0]
    tiles = place.shape[0]
    column_tile = pl.BlockSpec((share, TILE), lambda step, place: (0, place[step]))
    row_tile = pl.BlockSpec((TILE, width), lambda step, place: (step, 0))
    whole = pl.BlockSpec(
        slab.shape, lambda step, place: (0,) * 6, pipeline_mode=pl.Buffered(1)
    )
    operands = (place, slab, factor_rows, panel_rows, trailing)
    in_specs = [whole, row_tile, row_tile, column_tile]
    aliases = {}
    if previous is not None:
        operands += (previous,)
        in_specs.append(pl.BlockSpec(memory_space=pl.ANY))
        aliases = {5: 0}
    return pl.pallas_call(
        update_kernel,
        out_shape=jax.ShapeDtypeStruct(trailing.shape, trailing.dtype),
        grid_spec=pltpu.PrefetchScalarGridSpec(
            num_scalar_prefetch=1,
            grid=(tiles,),
            in_specs=in_specs,
            out_specs=column_tile,
            scratch_shapes=[
                pltpu.VMEM((share, 6 * width), jnp.bfloat16),
                pltpu.VMEM((TILE, 6 * width), jnp.bfloat16),
            ],
        ),
        input_output_aliases=aliases,
        compiler_params=pltpu.CompilerParams(vmem_limit_bytes=60 * 2**20),
        cost_estimate=pl.CostEstimate(
            flops=6 * tiles * TILE * rows * 2 * width,
            bytes_accessed=4 * (tiles * TILE * (2 * rows + 2 * width) + 2 * rows * width),
            transcendentals=0,
        ),
    )(*operands)


def bands_kernel(place, slab_ref, factor_ref, panel_ref, trailing_ref, _, out_ref, left, right):
    width = factor_ref.shape[1]

    @pl.when(pl.program_id(0) == 0)
    def _():
        for part, ref in enumerate((factor_ref, panel_ref)):
            top, low = split(ref[...])
            for slot, value in enumerate((top, low, top)):
                right[:, pl.ds((2 * slot + part) * width, width)] = value

    lay_slab(slab_ref, left)
    total = lax.dot_general(left[...], right[...], LANES, preferred_element_type=jnp.float32)
    out_ref[...] = trailing_ref[...] - total


def update_bands(place, slab, factor_rows, panel_rows, trailing, previous):
    groups, half, places, _, share, width = slab.shape
    pack = 2 if places % 2 == 0 else 1
    across = places // pack
    lines = half * pack * share
    columns = factor_rows.shape[0]
    rows = trailing.shape[0]
    tile = pl.BlockSpec((lines, columns), lambda step, place: (step, place[0]))
    fixed = pl.BlockSpec((columns, width), lambda step, place: (0, 0), pipeline_mode=pl.Buffered(1))
    return pl.pallas_call(
        bands_kernel,
        out_shape=jax.ShapeDtypeStruct(trailing.shape, trailing.dtype),
        grid_spec=pltpu.PrefetchScalarGridSpec(
            num_scalar_prefetch=1,
            grid=(groups * across,),
            in_specs=[
                pl.BlockSpec(
                    (1, half, pack, 2, share, width),
                    lambda step, place: (step // across, 0, step % across, 0, 0, 0),
                ),
                fixed,
                fixed,
                tile,
                pl.BlockSpec(memory_space=pl.ANY),
            ],
            out_specs=tile,
            scratch_shapes=[
                pltpu.VMEM((lines, 6 * width), jnp.bfloat16),
                pltpu.VMEM((columns, 6 * width), jnp.bfloat16),
            ],
        ),
        input_output_aliases={5: 0},
        compiler_params=pltpu.CompilerParams(vmem_limit_bytes=48 * 2**20),
        cost_estimate=pl.CostEstimate(
            flops=6 * columns * rows * 2 * width,
            bytes_accessed=4 * (columns * (2 * rows + 2 * width) + 2 * rows * width),
            transcendentals=0,
        ),
    )(place, slab, factor_rows, panel_rows, trailing, previous)


def corner_rows(corner_inverse, block, inverse):
    exact = lax.Precision.HIGHEST
    return contract(matmul(corner_inverse, block, exact), inverse, exact)


def plain(trailing, panel_block, factor_panel, corner_block, corner_inverse):
    slab = trailing.shape[0]
    sources = [lax.axis_index(a) == 0 for a in PLANE]

    def broadcast(value):
        return lax.psum(jnp.where(sources[0] & sources[1], value, 0.0), PLANE)

    block, inverse = corner_gather(corner_block, corner_inverse, 0)
    corner_out = corner_rows(corner_inverse, block, inverse)
    turned, panel_out = transform(panel_block, factor_panel, block, inverse)
    panel_cols = lax.all_gather(panel_block, "depth", axis=0, tiled=True)
    factor_cols = lax.all_gather(factor_panel, "depth", axis=0, tiled=True)
    panel_piece, turned_piece = broadcast(panel_out[:slab]), broadcast(turned[:slab])
    change = contract(panel_piece, factor_cols) + contract(turned_piece, panel_cols)
    return trailing - change, panel_out, corner_out


def paired(n_row, n_col, trailing, panel_block, factor_panel, corner_block, corner_inverse):
    slab = trailing.shape[0]
    count = panel_block.shape[0]
    lower = lax.axis_index("depth") == 0

    tiles = -(-2 * count // TILE)
    lead = -count % TILE
    full = (count - lead) // TILE - 1
    cut = lead + full * TILE
    early, late = {}, {}
    for name, value in (("factor", factor_panel), ("panel", panel_block)):
        early[name] = lax.ppermute(value[:cut], "depth", SWAP)
        late[name] = lax.ppermute(value[cut:], "depth", SWAP)

    block, inverse = corner_gather(corner_block, corner_inverse, 2)
    piece = slab_piece(panel_block, factor_panel, slab, n_row, n_col)
    piece_turned, piece_panel, corner_out = transform_with_corner(
        piece[0], piece[1], corner_inverse, block, inverse
    )
    slab_rows = lax.all_gather(jnp.stack([piece_panel, piece_turned]), PLANE, axis=0)
    slab_rows = slab_rows.reshape(2, n_row // 2, n_col, *slab_rows.shape[1:])

    _, panel_out = transform(panel_block, factor_panel, block, inverse)

    def padded(rows, size):
        value = jnp.concatenate(rows)
        return jnp.pad(value, ((0, size - value.shape[0]), (0, 0)))

    upper = -(-count // TILE)
    first_low = (count + cut) // TILE
    first_tiles = full + tiles - upper
    assert first_low == first_tiles
    last_tiles = tiles - first_tiles

    def first_rows(own, part):
        size = first_tiles * TILE
        low = padded([own, part], size)
        high = padded([part[: full * TILE], own[lead:]], size)
        return jnp.where(lower, low, high)

    def last_rows(own, part, rest):
        size = last_tiles * TILE
        low = padded([rest], size)
        high = padded([part[full * TILE :], rest, own[:lead]], size)
        return jnp.where(lower, low, high)

    low_order = jnp.arange(tiles)
    high_order = jnp.concatenate(
        [jnp.arange(full), jnp.arange(upper, tiles), jnp.arange(full, upper)]
    )
    order = jnp.where(lower, low_order, high_order).astype(jnp.int32)
    factor_rows = first_rows(factor_panel, early["factor"])
    panel_rows = first_rows(panel_block, early["panel"])
    out = update(order[:first_tiles], slab_rows, factor_rows, panel_rows, trailing, None)
    factor_rows = last_rows(factor_panel, early["factor"], late["factor"])
    panel_rows = last_rows(panel_block, early["panel"], late["panel"])
    place = order[first_tiles:]
    if full % last_tiles == 0 and first_low % last_tiles == 0 and upper - full == last_tiles:
        out = update_bands(place[:1] // last_tiles, slab_rows, factor_rows, panel_rows, trailing, out)
    else:
        out = update(place, slab_rows, factor_rows, panel_rows, trailing, out)
    return out, panel_out, corner_out


def paired_fits(n_row, n_depth, trailing, panel_block):
    count = panel_block.shape[0]
    fits = trailing.shape[1] == 2 * count and trailing.shape[0] <= count
    return n_depth == 2 and n_row % 2 == 0 and fits and count % 32 == 0 and count >= 4 * TILE


def body(n_row, n_col, n_depth, trailing, panel_block, *rest):
    if paired_fits(n_row, n_depth, trailing, panel_block):
        return paired(n_row, n_col, trailing, panel_block, *rest)
    return plain(trailing, panel_block, *rest)


def solution(mesh):
    in_specs = (P("depth", PLANE),) + (P(ALL, None),) * 4
    out_specs = (P("depth", PLANE), P(ALL, None), P(ALL, None))
    sizes = [mesh.shape[a] for a in ALL]
    return jax.shard_map(
        functools.partial(body, *sizes),
        mesh=mesh,
        in_specs=in_specs,
        out_specs=out_specs,
        check_vma=False,
    )
```
